32 devices in a mesh: dp: 4 (over z), sx: 4 (over y, core), sy: 2 (over x).
Axes of the slice: x: 2, y: 2, z: 4, core: 2. Of those that a mesh axis runs over, the one named last changes fastest.
Arguments:
- volume: bfloat16 [4, 4, 16, 16, 128], P('dp', None, 'sx', 'sy'), may hold values from -6 to 6
- first_weight: bfloat16 [32, 108], replicated, may hold values from -0.625 to 0.625
- second_weight: bfloat16 [64, 864], replicated, may hold values from -0.21875 to 0.21875
- cotangent: bfloat16 [4, 64, 8, 8, 64], P('dp', None, 'sx', 'sy'), may hold values from -6 to 6
Outputs:
- grad_first: float32 [32, 108], replicated
- grad_second: float32 [64, 864], replicated
The draws below stay inside these ranges and needn't reach their ends.
All inputs are finite; a program needn't handle non-finite values.
Results may differ from the reference program's by a relative error of at most 0.014.
Values may be sent and summed in bfloat16 or wider, within the bound.
A program may use at most 64 MiB of HBM per device.

```python
import jax
import jax.numpy as jnp
from jax import lax

C_IN = 4
C1 = 32
C2 = 64
CZ = 128
BATCH = 4
NX = 16
NY = 16


def shard_levels(rng, extent, cuts, least, largest):
    factor_of = 1.0
    for axis_at, shards_of in cuts:
        heights = jax.random.uniform(jax.random.fold_in(jax.random.fold_in(rng, 6), axis_at), (shards_of,), jnp.float32, least / len(cuts), largest / len(cuts))
        factor_of = factor_of * jnp.repeat(jnp.exp(heights), extent[axis_at] // shards_of).reshape((-1,) + (1,) * (len(extent) - 1 - axis_at))
    return factor_of


def bell_draw(rng, dims, width, limit, split=(), dtype=jnp.bfloat16):
    values = width * jax.random.normal(rng, dims, jnp.float32)
    if split:
        values = values * shard_levels(rng, dims, split, -0.22, 0.18)
    return jnp.clip(values, -limit, limit).astype(dtype)


def setup_inputs(seed: int = 0) -> dict:
    streams_of = jax.random.split(jax.random.key(seed), 5)
    volume = bell_draw(streams_of[0], (BATCH, C_IN, NX, NY, CZ), 1.0, 6.0, ((0, 4), (2, 4), (3, 2)))
    first_weight = bell_draw(streams_of[1], (C1, 27 * C_IN), (27 * C_IN) ** -0.5, 0.625)
    second_weight = bell_draw(streams_of[2], (C2, 27 * C1), (27 * C1) ** -0.5, 0.21875)
    cotangent = bell_draw(streams_of[3], (BATCH, C2, NX // 2, NY // 2, CZ // 2), 1.0, 6.0, ((0, 4), (2, 4), (3, 2)))
    return dict(volume=volume, first_weight=first_weight, second_weight=second_weight, cotangent=cotangent)


def leaky(value):
    return 0.3 * value + 0.7 * jax.nn.softplus(value)

def slope(value):
    return 0.3 + 0.7 * jax.nn.sigmoid(value)

def patches(padded, width_x, width_y, width_z):
    columns = []
    for shift_x in range(3):
        for shift_y in range(3):
            for shift_z in range(3):
                columns.append(padded[:, shift_x:shift_x + width_x, shift_y:shift_y + width_y, shift_z:shift_z + width_z])
    stacked = jnp.concatenate(columns, 0)
    return stacked.reshape(stacked.shape[0], width_x * width_y * width_z)

def pad_all(field):
    return jnp.pad(field, ((0, 0), (1, 1), (1, 1), (1, 1)))

def one_sample(first_weight, second_weight, sample, cot):
    chans, width_x, width_y, width_z = sample.shape
    fine_cols = patches(pad_all(sample), width_x, width_y, width_z)
    pre_first = jnp.dot(first_weight, fine_cols, preferred_element_type=jnp.float32)
    hidden = leaky(pre_first).astype(jnp.bfloat16)
    inner = hidden.shape[0]
    half_x, half_y, half_z = (width_x // 2, width_y // 2, width_z // 2)
    pooled = (hidden.astype(jnp.float32).reshape(inner, half_x, 2, half_y, 2, half_z, 2).sum(axis=(2, 4, 6)) * 0.125).astype(jnp.bfloat16)
    coarse_cols = patches(pad_all(pooled), half_x, half_y, half_z)
    pre_second = jnp.dot(second_weight, coarse_cols, preferred_element_type=jnp.float32)
    outer = pre_second.shape[0]
    back = (cot.reshape(outer, -1).astype(jnp.float32) * slope(pre_second)).astype(jnp.bfloat16)
    second_part = lax.dot_general(back, coarse_cols, (((1,), (1,)), ((), ())), preferred_element_type=jnp.float32)
    back_cols = patches(pad_all(back.reshape(outer, half_x, half_y, half_z)), half_x, half_y, half_z)
    mirrored = second_weight.reshape(outer, 27, inner)[:, ::-1, :].transpose(2, 1, 0).reshape(inner, 27 * outer)
    up = jnp.dot(mirrored, back_cols, preferred_element_type=jnp.float32)
    spread = jnp.broadcast_to(up.reshape(inner, half_x, 1, half_y, 1, half_z, 1), (inner, half_x, 2, half_y, 2, half_z, 2)).reshape(inner, -1)
    lower = (spread * 0.125 * slope(pre_first)).astype(jnp.bfloat16)
    first_part = lax.dot_general(lower, fine_cols, (((1,), (1,)), ((), ())), preferred_element_type=jnp.float32)
    return (first_part, second_part)

def reference(volume, first_weight, second_weight, cotangent):

    def step(pair):
        return one_sample(first_weight, second_weight, pair[0], pair[1])
    firsts, seconds = lax.map(step, (volume, cotangent))
    coarse_count = volume.shape[0] * volume.shape[2] * volume.shape[3] * volume.shape[4] // 8
    scale_second = 1.0 / jnp.sqrt(jnp.float32(coarse_count))
    scale_first = 1.0 / jnp.sqrt(jnp.float32(coarse_count * 8))
    return (lax.optimization_barrier(jnp.sum(firsts, 0)) * scale_first, lax.optimization_barrier(jnp.sum(seconds, 0)) * scale_second)
```

```python
import functools

import jax
import jax.numpy as jnp
from jax import lax
from jax.experimental import pallas as pl
from jax.experimental.pallas import tpu as pltpu
from jax.sharding import PartitionSpec as P

F32 = jnp.float32
BF16 = jnp.bfloat16
MESH = pl.DeviceIdType.MESH
DIRS = [(dx, dy) for dx in (-1, 0, 1) for dy in (-1, 0, 1) if (dx, dy) != (0, 0)]


def nt(a, b):
    return lax.dot_general(a, b, (((1,), (1,)), ((), ())), preferred_element_type=F32)


def nn(a, b):
    return jnp.dot(a, b, preferred_element_type=F32)


def iota(shape, dim):
    return lax.broadcasted_iota(jnp.int32, shape, dim)


def one_hot(cond):
    return jnp.where(cond, 1.0, 0.0).astype(BF16)


def slope(value):
    return 0.65 + 0.35 * jnp.tanh(0.5 * value)


def leaky(value):
    tail = jnp.log(1.0 + jnp.exp(-jnp.abs(value)))
    return 0.3 * value + 0.7 * (jnp.maximum(value, 0.0) + tail)


def kernel(
    nd, nx, ny,
    vol, w1, w2, cot,
    out1, out2,
    rows_f, vs, cot_f, cot_d, pool, q, bk, bs, slope1, w2t,
    g2s, g2r, g2d, ag, g1p, g1d,
    halo_send, halo_recv, plane_send, plane_recv, dp_send, dp_recv,
):
    dpi, ix, iy = lax.axis_index("dp"), lax.axis_index("sx"), lax.axis_index("sy")
    n_plane = nx * ny
    me = ix * ny + iy
    chans, X, Y, Z = vol.shape[1:]
    hx, hy, hz = X // 2, Y // 2, Z // 2
    inner, outer = w1.shape[0], w2.shape[0]
    rows = outer // n_plane
    taps = 3 * chans
    tap_rows = vs.shape[2]

    vs[...] = jnp.zeros_like(vs)
    pool[...] = jnp.zeros_like(pool)
    bk[...] = jnp.zeros_like(bk)

    def plane_id(r):
        peer = lax.rem(me + r, n_plane)
        return {"sx": peer // ny, "sy": lax.rem(peer, ny)}

    def dp_id(r):
        return {"dp": lax.rem(dpi + r, nd)}

    barrier = pltpu.get_barrier_semaphore()
    for r in range(1, n_plane):
        pl.semaphore_signal(barrier, inc=1, device_id=plane_id(r), device_id_type=MESH)
    for r in range(1, nd):
        pl.semaphore_signal(barrier, inc=1, device_id=dp_id(r), device_id_type=MESH)

    rows_f[...] = jnp.zeros_like(rows_f)
    lane = iota((Y, Z), 1)
    for c in range(chans):
        for x in range(X):
            v = vol[0, c, x].astype(F32)
            down = jnp.where(lane == 0, 0.0, pltpu.roll(v, 1, 1))
            up_z = jnp.where(lane == Z - 1, 0.0, pltpu.roll(v, Z - 1, 1))
            for e, moved in enumerate((down, v, up_z)):
                rows_f[pl.ds(x * Y * tap_rows + e * chans + c, Y, stride=tap_rows), :] = moved
    for x in range(X):
        for y in range(Y):
            start = (x * Y + y) * tap_rows
            vs[1 + x, 1 + y] = rows_f[start : start + tap_rows].astype(BF16)

    pl.semaphore_wait(barrier, n_plane - 1 + nd - 1)

    def there(dx, dy):
        ok = None
        for d, i, n in ((dx, ix, nx), (dy, iy, ny)):
            if d == 0:
                continue
            here = (i + d >= 0) & (i + d < n)
            ok = here if ok is None else ok & here
        return ok

    def side(d, n):
        if d == 0:
            return pl.ds(1, n), pl.ds(1, n)
        return (pl.ds(1, 1), pl.ds(n + 1, 1)) if d < 0 else (pl.ds(n, 1), pl.ds(0, 1))

    def halo(ref, stage):
        wide, high = ref.shape[0] - 2, ref.shape[1] - 2
        copies = []
        for i, (dx, dy) in enumerate(DIRS):
            (sx, tx), (sy, ty) = side(dx, wide), side(dy, high)
            copy = pltpu.make_async_remote_copy(
                src_ref=ref.at[sx, sy],
                dst_ref=ref.at[tx, ty],
                send_sem=halo_send.at[stage, i],
                recv_sem=halo_recv.at[stage, i],
                device_id={"sx": ix + dx, "sy": iy + dy},
                device_id_type=MESH,
            )
            pl.when(there(dx, dy))(copy.start)
            copies.append((copy, dx, dy))
        return copies

    def halo_arrived(copies):
        for copy, dx, dy in copies:
            pl.when(there(-dx, -dy))(copy.wait_recv)

    def halo_sent(copies):
        for copy, dx, dy in copies:
            pl.when(there(dx, dy))(copy.wait_send)

    def spread(count, ids, src, dst, send, recv, stage):
        copies = []
        for r in range(1, count):
            copy = pltpu.make_async_remote_copy(
                src_ref=src(r),
                dst_ref=dst,
                send_sem=send.at[stage, r],
                recv_sem=recv.at[stage, r],
                device_id=ids(r),
                device_id_type=MESH,
            )
            copy.start()
            copies.append(copy)
        return copies

    sent = []
    halos = [halo(vs, 0)]

    n12 = 9 * taps
    pick_r, pick_c = iota((n12, 9 * tap_rows), 0), iota((n12, 9 * tap_rows), 1)
    tap = lax.rem(pick_c, tap_rows)
    pick = one_hot((pick_r == (pick_c // tap_rows) * taps + tap) & (tap < taps))
    w1p = nn(w1[...], pick).astype(BF16)
    eye = one_hot(iota((128, 128), 0) == iota((128, 128), 1))
    width = w2.shape[1]
    for at in range(0, width, 128):
        n = min(128, width - at)
        w2t[at : at + n] = nt(eye[:n, :n], w2[:, at : at + n]).astype(BF16)
    for o in range(outer):
        for x in range(hx):
            start = (o * hx + x) * hy
            cot_f[start : start + hy] = cot[0, o, x].astype(F32)
    cells = hx * hy
    stack = jnp.concatenate(
        [cot_f[pl.ds(i, outer, stride=cells), :] for i in range(cells)], axis=0
    ).astype(BF16)
    double = one_hot(iota((hz, Z), 0) == iota((hz, Z), 1) // 2)
    doubled = nn(stack, double)
    for i in range(cells):
        cot_d[:, i * Z : (i + 1) * Z] = doubled[i * outer : (i + 1) * outer]
    pool_m = one_hot(lax.rem(iota((4 * Z, Z), 0), Z) // 2 == iota((4 * Z, Z), 1) // 2)
    t_in, t_out = iota((Z, 2 * Z), 0), iota((Z, 2 * Z), 1)
    shift_m = one_hot(t_in == jnp.where(t_out < Z, t_out - 2, t_out - Z + 2))

    halo_arrived(halos[0])

    def fine_cols(x):
        return jnp.concatenate(
            [
                jnp.concatenate([vs[x + a, y + b] for y in range(Y)], axis=1)
                for a in range(3)
                for b in range(3)
            ],
            axis=0,
        )

    for xc in range(hx):
        hid = []
        for x in (2 * xc, 2 * xc + 1):
            pre = nn(w1p, fine_cols(x))
            slope1[x] = pre
            hid.append(leaky(pre).astype(BF16))
        block = jnp.concatenate(
            [
                jnp.concatenate(
                    [
                        hid[i][:, (2 * yc + j) * Z : (2 * yc + j + 1) * Z]
                        for i in range(2)
                        for j in range(2)
                    ],
                    axis=1,
                )
                for yc in range(hy)
            ],
            axis=0,
        )
        mean = (nn(block, pool_m) * 0.125).astype(BF16)
        for yc in range(hy):
            pool[1 + xc, 1 + yc] = mean[yc * inner : (yc + 1) * inner]
    halos.append(halo(pool, 1))

    inside = [(x, y) for x in range(1, hx + 1) for y in range(1, hy + 1)]
    rim = [
        (x, y) for x in range(hx + 2) for y in range(hy + 2) if (x, y) not in inside
    ]

    def shifts(src, dst, places, order):
        n = src.shape[2]
        tiles = jnp.concatenate([src[x, y] for x, y in places], axis=0)
        moved = nn(tiles, shift_m).astype(BF16)
        for i, (x, y) in enumerate(places):
            part = moved[i * n : (i + 1) * n]
            dst[x, y, order[0] * n : (order[0] + 1) * n] = part[:, :Z]
            dst[x, y, n : 2 * n] = tiles[i * n : (i + 1) * n]
            dst[x, y, order[1] * n : (order[1] + 1) * n] = part[:, Z:]

    for x in range(X):
        slope1[x] = slope(slope1[x]) * 0.125
    shifts(pool, q, inside, (0, 2))
    halo_arrived(halos[1])
    shifts(pool, q, rim, (0, 2))

    places = [(x, y) for x in range(hx) for y in range(hy)]

    def coarse_cols():
        return jnp.concatenate(
            [
                jnp.concatenate([q[x + a, y + b] for x, y in places], axis=1)
                for a in range(3)
                for b in range(3)
            ],
            axis=0,
        )

    pre_second = nn(w2[...], coarse_cols())
    back = (cot_d[...] * slope(pre_second)).astype(BF16)
    for i, (x, y) in enumerate(places):
        bk[1 + x, 1 + y] = back[:, i * Z : (i + 1) * Z]
    halos.append(halo(bk, 2))

    count = cells * hz * nd * n_plane
    scale_second, scale_first = count**-0.5, (8 * count) ** -0.5
    grad2 = nt(back, coarse_cols()) * (0.5 * scale_second)
    for i in range(n_plane):
        g2s[i] = grad2[i * rows : (i + 1) * rows].astype(BF16)
    g2r[me] = g2s[me]
    in_plane = lambda r: g2s.at[lax.rem(me + r, n_plane)]
    scatter = spread(n_plane, plane_id, in_plane, g2r.at[me], plane_send, plane_recv, 0)
    sent += scatter

    shifts(bk, bs, inside, (2, 0))
    halo_arrived(halos[2])
    shifts(bk, bs, rim, (2, 0))
    total = jnp.zeros((inner, cells * Z), F32)
    for a in range(3):
        for b in range(3):
            for e in range(3):
                k = (a * 3 + b) * 3 + e
                rhs = jnp.concatenate(
                    [
                        bs[x + 2 - a, y + 2 - b, e * outer : (e + 1) * outer]
                        for x, y in places
                    ],
                    axis=1,
                )
                total = total + nn(w2t[k * inner : (k + 1) * inner], rhs)

    for copy in scatter:
        copy.wait_recv()
    acc = jnp.zeros((rows, width), F32)
    for i in range(n_plane):
        acc = acc + g2r[i].astype(F32)
    g2d[dpi] = acc.astype(BF16)
    own = lambda ref, i: (lambda r: ref.at[i])
    across = spread(nd, dp_id, own(g2d, dpi), g2d.at[dpi], dp_send, dp_recv, 0)
    sent += across

    grad1 = jnp.zeros((inner, 9 * tap_rows), F32)
    for x in range(X):
        lower = []
        for y in range(Y):
            at = ((x // 2) * hy + y // 2) * Z
            lower.append(total[:, at : at + Z] * slope1[x, :, y * Z : (y + 1) * Z])
        low = jnp.concatenate(lower, axis=1).astype(BF16)
        grad1 = grad1 + nt(low, fine_cols(x))
    grad1 = nt((grad1 * scale_first).astype(BF16), pick)
    g1p[me] = grad1.astype(BF16)
    firsts = spread(n_plane, plane_id, own(g1p, me), g1p.at[me], plane_send, plane_recv, 1)
    sent += firsts

    for copy in across:
        copy.wait_recv()
    acc = jnp.zeros((rows, width), F32)
    for i in range(nd):
        acc = acc + g2d[i].astype(F32)
    ag[me] = acc.astype(BF16)
    gather = spread(n_plane, plane_id, own(ag, me), ag.at[me], plane_send, plane_recv, 2)
    sent += gather

    for copy in firsts:
        copy.wait_recv()
    acc = jnp.zeros(out1.shape, F32)
    for i in range(n_plane):
        acc = acc + g1p[i].astype(F32)
    g1d[dpi] = acc.astype(BF16)
    last = spread(nd, dp_id, own(g1d, dpi), g1d.at[dpi], dp_send, dp_recv, 1)
    sent += last

    for copy in gather:
        copy.wait_recv()
    for i in range(n_plane):
        out2[i * rows : (i + 1) * rows] = ag[i].astype(F32)
    for copy in last:
        copy.wait_recv()
    acc = jnp.zeros(out1.shape, F32)
    for i in range(nd):
        acc = acc + g1d[i].astype(F32)
    out1[...] = acc
    for copies in halos:
        halo_sent(copies)
    for copy in sent:
        copy.wait_send()


def shards(nd, nx, ny, volume, first_weight, second_weight, cotangent):
    _, chans, X, Y, Z = volume.shape
    inner, outer = first_weight.shape[0], second_weight.shape[0]
    width = second_weight.shape[1]
    hx, hy, hz = X // 2, Y // 2, Z // 2
    cells = hx * hy
    n_plane = nx * ny
    rows = outer // n_plane
    tap_rows = -(-3 * chans // 16) * 16
    vmem = pl.BlockSpec(memory_space=pltpu.VMEM)
    dma = pltpu.SemaphoreType.DMA
    return pl.pallas_call(
        functools.partial(kernel, nd, nx, ny),
        out_shape=(
            jax.ShapeDtypeStruct(first_weight.shape, F32),
            jax.ShapeDtypeStruct(second_weight.shape, F32),
        ),
        in_specs=[vmem] * 4,
        out_specs=(vmem, vmem),
        scratch_shapes=[
            pltpu.VMEM((X * Y * tap_rows, Z), F32),
            pltpu.VMEM((X + 2, Y + 2, tap_rows, Z), BF16),
            pltpu.VMEM((outer * cells, hz), F32),
            pltpu.VMEM((outer, cells * Z), F32),
            pltpu.VMEM((hx + 2, hy + 2, inner, Z), BF16),
            pltpu.VMEM((hx + 2, hy + 2, 3 * inner, Z), BF16),
            pltpu.VMEM((hx + 2, hy + 2, outer, Z), BF16),
            pltpu.VMEM((hx + 2, hy + 2, 3 * outer, Z), BF16),
            pltpu.VMEM((X, inner, Y * Z), F32),
            pltpu.VMEM((width, outer), BF16),
            pltpu.VMEM((n_plane, rows, width), BF16),
            pltpu.VMEM((n_plane, rows, width), BF16),
            pltpu.VMEM((nd, rows, width), BF16),
            pltpu.VMEM((n_plane, rows, width), BF16),
            pltpu.VMEM((n_plane,) + first_weight.shape, BF16),
            pltpu.VMEM((nd,) + first_weight.shape, BF16),
            dma((3, 8)),
            dma((3, 8)),
            dma((3, n_plane)),
            dma((3, n_plane)),
            dma((2, nd)),
            dma((2, nd)),
        ],
        compiler_params=pltpu.CompilerParams(
            collective_id=0, has_side_effects=True, vmem_limit_bytes=48 * 1024 * 1024
        ),
        name="step",
    )(volume, first_weight, second_weight, cotangent)


def solution(mesh):
    sizes = dict(mesh.shape)
    return jax.shard_map(
        functools.partial(shards, sizes["dp"], sizes["sx"], sizes["sy"]),
        mesh=mesh,
        in_specs=(P("dp", None, "sx", "sy", None), P(), P(), P("dp", None, "sx", "sy", None)),
        out_specs=(P(), P()),
        check_vma=False,
    )
```

```python
import functools

import jax
import jax.numpy as jnp
from jax import lax
from jax.experimental import pallas as pl
from jax.experimental.pallas import tpu as pltpu
from jax.sharding import PartitionSpec as P

F32 = jnp.float32
BF16 = jnp.bfloat16
MESH = pl.DeviceIdType.MESH
REACH = 3
DIRS = [(dx, dy) for dx in (-1, 0, 1) for dy in (-1, 0, 1) if (dx, dy) != (0, 0)]


def nt(a, b):
    return lax.dot_general(a, b, (((1,), (1,)), ((), ())), preferred_element_type=F32)


def nn(a, b):
    return jnp.dot(a, b, preferred_element_type=F32)


def iota(shape, dim):
    return lax.broadcasted_iota(jnp.int32, shape, dim)


def one_hot(cond):
    return jnp.where(cond, 1.0, 0.0).astype(BF16)


def slope(value):
    return 0.65 + 0.35 * jnp.tanh(0.5 * value)


def leaky(value):
    tail = jnp.log(1.0 + jnp.exp(-jnp.abs(value)))
    return 0.3 * value + 0.7 * (jnp.maximum(value, 0.0) + tail)


def kernel(
    nd, nx, ny,
    vol_h, w1_h, w2_h, cot_h,
    out1, out2,
    vol, w1, w2, cot,
    raw, rows_f, vs, cot_f, cot_d, q, ups, slope1, w2t,
    g2s, g2r, g2d, ag, g1p, g1d,
    halo_send, halo_recv, plane_send, plane_recv, dp_send, dp_recv, fetch_sem,
):
    fetches = [
        pltpu.make_async_copy(src, dst, fetch_sem.at[i])
        for i, (src, dst) in enumerate(((vol_h, vol), (w1_h, w1), (w2_h, w2), (cot_h, cot)))
    ]
    for fetch in fetches:
        fetch.start()
    dpi, ix, iy = lax.axis_index("dp"), lax.axis_index("sx"), lax.axis_index("sy")
    n_plane = nx * ny
    me = ix * ny + iy
    chans, X, Y, Z = vol.shape[1:]
    hx, hy, hz = X // 2, Y // 2, Z // 2
    inner, outer = w1.shape[0], w2.shape[0]
    rows = outer // n_plane
    taps = 3 * chans
    tap_rows = vs.shape[2]

    raw[...] = jnp.zeros_like(raw)

    def plane_id(r):
        peer = lax.rem(me + r, n_plane)
        return {"sx": peer // ny, "sy": lax.rem(peer, ny)}

    def dp_id(r):
        return {"dp": lax.rem(dpi + r, nd)}

    barrier = pltpu.get_barrier_semaphore()
    for r in range(1, n_plane):
        pl.semaphore_signal(barrier, inc=1, device_id=plane_id(r), device_id_type=MESH)
    for r in range(1, nd):
        pl.semaphore_signal(barrier, inc=1, device_id=dp_id(r), device_id_type=MESH)

    def inside(d, i, n):
        return (i + d >= 0) & (i + d < n)

    def there(dx, dy):
        if dx == 0:
            return inside(dy, iy, ny)
        if dy == 0:
            return inside(dx, ix, nx)
        return inside(dx, ix, nx) & inside(dy, iy, ny)

    def xs(dx):
        return {-1: range(X - REACH, X), 0: range(X), 1: range(REACH)}[dx]

    halos = []
    for i, (dx, dy) in enumerate(DIRS):
        span = xs(-dx)
        part = pl.ds(span[0], len(span))
        copy = pltpu.make_async_remote_copy(
            src_ref=vol.at[0, :, part],
            dst_ref=raw.at[DIRS.index((-dx, -dy)), :, part],
            send_sem=halo_send.at[i],
            recv_sem=halo_recv.at[i],
            device_id={"sx": ix + dx, "sy": iy + dy},
            device_id_type=MESH,
        )
        halos.append((copy, dx, dy))

    rows_f[...] = jnp.zeros_like(rows_f)
    fetches[0].wait()
    pl.semaphore_wait(barrier, n_plane - 1 + nd - 1)
    for copy, dx, dy in halos:
        pl.when(there(dx, dy))(copy.start)

    def spread(count, ids, src, dst, send, recv, stage):
        copies = []
        for r in range(1, count):
            copy = pltpu.make_async_remote_copy(
                src_ref=src(r),
                dst_ref=dst,
                send_sem=send.at[stage, r],
                recv_sem=recv.at[stage, r],
                device_id=ids(r),
                device_id_type=MESH,
            )
            copy.start()
            copies.append(copy)
        return copies

    lane = iota((Y, Z), 1)

    def lay(src, dx, dy):
        for c in range(chans):
            for x in xs(dx):
                v = src(c, x).astype(F32)
                down = jnp.where(lane == 0, 0.0, pltpu.roll(v, 1, 1))
                up_z = jnp.where(lane == Z - 1, 0.0, pltpu.roll(v, Z - 1, 1))
                first = ((x + dx * X + REACH) * 3 + dy + 1) * Y
                for e, moved in enumerate((down, v, up_z)):
                    at = first * tap_rows + e * chans + c
                    rows_f[pl.ds(at, Y, stride=tap_rows), :] = moved

    def pack(x, y):
        start = (x * 3 * Y + y + Y - REACH) * tap_rows
        vs[x, y] = rows_f[start : start + tap_rows].astype(BF16)

    lay(lambda c, x: vol[0, c, x], 0, 0)
    own = [(x, y) for x in range(REACH, X + REACH) for y in range(REACH, Y + REACH)]
    for x, y in own:
        pack(x, y)
    for fetch in fetches[1:]:
        fetch.wait()
    n12 = 9 * taps
    pick_r, pick_c = iota((n12, 9 * tap_rows), 0), iota((n12, 9 * tap_rows), 1)
    tap = lax.rem(pick_c, tap_rows)
    pick = one_hot((pick_r == (pick_c // tap_rows) * taps + tap) & (tap < taps))
    w1p = nn(w1[...], pick).astype(BF16)
    eye = one_hot(iota((128, 128), 0) == iota((128, 128), 1))
    width = w2.shape[1]
    for at in range(0, width, 128):
        n = min(128, width - at)
        w2t[at : at + n] = nt(eye[:n, :n], w2[:, at : at + n]).astype(BF16)
    for o in range(outer):
        for x in range(hx):
            start = (o * hx + x) * hy
            cot_f[start : start + hy] = cot[0, o, x].astype(F32)
    cells = hx * hy
    stack = jnp.concatenate(
        [cot_f[pl.ds(i, outer, stride=cells), :] for i in range(cells)], axis=0
    ).astype(BF16)
    double = one_hot(iota((hz, Z), 0) == iota((hz, Z), 1) // 2)
    doubled = nn(stack, double)
    for i in range(cells):
        cot_d[:, i * Z : (i + 1) * Z] = doubled[i * outer : (i + 1) * outer]
    p_in, p_out = iota((4 * Z, 3 * Z), 0), iota((4 * Z, 3 * Z), 1)
    pool_m = one_hot(
        lax.rem(p_in, Z) // 2 == lax.rem(p_out, Z) // 2 + p_out // Z - 1
    )
    t_in, t_out = iota((Z, 2 * Z), 0), iota((Z, 2 * Z), 1)
    shift_m = one_hot(t_in == jnp.where(t_out < Z, t_out + 2, t_out - Z - 2))

    def present(d, i, n):
        return jnp.where(inside(d, i, n), 1.0, 0.0) if d else 1.0

    in_x = {d: present(d, ix, nx) for d in (-1, 0, 1)}
    in_y = {d: present(d, iy, ny) for d in (-1, 0, 1)}

    def part_of(at, rim, size):
        return -1 if at < rim else (1 if at >= rim + size else 0)

    def masked(value, at_x, at_y):
        if at_x:
            value = value * in_x[at_x]
        if at_y:
            value = value * in_y[at_y]
        return value

    for copy, dx, dy in halos:
        pl.when(there(-dx, -dy))(copy.wait_recv)
    for i, (dx, dy) in enumerate(DIRS):
        lay(lambda c, x, i=i: raw[i, c, x], dx, dy)
    for x in range(X + 2 * REACH):
        for y in range(Y + 2 * REACH):
            if (x, y) not in own:
                pack(x, y)

    wide, high = X + 4, Y + 4

    def fine_cols(x):
        return jnp.concatenate(
            [
                jnp.concatenate([vs[x + a, y + b] for y in range(high)], axis=1)
                for a in range(3)
                for b in range(3)
            ],
            axis=0,
        )

    for xc in range(hx + 2):
        hid = []
        for x in (2 * xc, 2 * xc + 1):
            pre = nn(w1p, fine_cols(x))
            slope1[x] = pre
            hid.append(leaky(pre).astype(BF16))
        block = jnp.concatenate(
            [
                jnp.concatenate(
                    [
                        hid[i][:, (2 * yc + j) * Z : (2 * yc + j + 1) * Z]
                        for i in range(2)
                        for j in range(2)
                    ],
                    axis=1,
                )
                for yc in range(hy + 2)
            ],
            axis=0,
        )
        mean = nn(block, pool_m) * 0.125
        for yc in range(hy + 2):
            tile = mean[yc * inner : (yc + 1) * inner]
            tile = masked(tile, part_of(xc, 1, hx), part_of(yc, 1, hy)).astype(BF16)
            for e in range(3):
                q[xc, yc, e * inner : (e + 1) * inner] = tile[:, e * Z : (e + 1) * Z]

    places = [(x, y) for x in range(hx) for y in range(hy)]

    def coarse_cols():
        return jnp.concatenate(
            [
                jnp.concatenate([q[x + a, y + b] for x, y in places], axis=1)
                for a in range(3)
                for b in range(3)
            ],
            axis=0,
        )

    pre_second = nn(w2[...], coarse_cols())
    back = (cot_d[...] * slope(pre_second)).astype(BF16)

    count = cells * hz * nd * n_plane
    scale_second, scale_first = count**-0.5, (8 * count) ** -0.5
    grad2 = nt(back, coarse_cols()) * (0.5 * scale_second)
    for i in range(n_plane):
        g2s[i] = grad2[i * rows : (i + 1) * rows].astype(BF16)
    g2r[me] = g2s[me]
    in_plane = lambda r: g2s.at[lax.rem(me + r, n_plane)]
    scatter = spread(n_plane, plane_id, in_plane, g2r.at[me], plane_send, plane_recv, 0)
    sent = list(scatter)

    tiles = jnp.concatenate([back[:, i * Z : (i + 1) * Z] for i in range(cells)], axis=0)
    moved = nn(tiles, shift_m).astype(BF16)

    def flat(value, half):
        return jnp.concatenate(
            [
                value[i * outer : (i + 1) * outer, half * Z : (half + 1) * Z]
                for i in range(cells)
            ],
            axis=1,
        )

    share = None
    for e, rhs in enumerate((flat(moved, 0), back, flat(moved, 1))):
        lhs = jnp.concatenate(
            [w2t[(3 * ab + e) * inner : (3 * ab + e + 1) * inner] for ab in range(9)],
            axis=0,
        )
        term = nn(lhs, rhs)
        share = term if share is None else share + term
    for xe in range(hx + 2):
        for ye in range(hy + 2):
            total = None
            for a in range(3):
                for b in range(3):
                    x, y = xe - a, ye - b
                    if 0 <= x < hx and 0 <= y < hy:
                        ab, at = 3 * a + b, (x * hy + y) * Z
                        term = share[ab * inner : (ab + 1) * inner, at : at + Z]
                        total = term if total is None else total + term
            ups[xe, ye] = masked(total * 0.125, part_of(xe, 1, hx), part_of(ye, 1, hy))

    for x in range(wide):
        slope1[x] = slope(slope1[x])

    for copy in scatter:
        copy.wait_recv()
    acc = jnp.zeros((rows, width), F32)
    for i in range(n_plane):
        acc = acc + g2r[i].astype(F32)
    g2d[dpi] = acc.astype(BF16)
    held = lambda ref, i: (lambda r: ref.at[i])
    across = spread(nd, dp_id, held(g2d, dpi), g2d.at[dpi], dp_send, dp_recv, 0)
    sent += across

    grad1 = jnp.zeros((inner, 9 * tap_rows), F32)
    for x in range(wide):
        low = jnp.concatenate(
            [ups[x // 2, y // 2] * slope1[x, :, y * Z : (y + 1) * Z] for y in range(high)],
            axis=1,
        ).astype(BF16)
        grad1 = grad1 + nt(low, fine_cols(x))
    grad1 = nt((grad1 * scale_first).astype(BF16), pick)
    g1p[me] = grad1.astype(BF16)
    firsts = spread(n_plane, plane_id, held(g1p, me), g1p.at[me], plane_send, plane_recv, 1)
    sent += firsts

    for copy in across:
        copy.wait_recv()
    acc = jnp.zeros((rows, width), F32)
    for i in range(nd):
        acc = acc + g2d[i].astype(F32)
    ag[me] = acc.astype(BF16)
    gather = spread(n_plane, plane_id, held(ag, me), ag.at[me], plane_send, plane_recv, 2)
    sent += gather

    for copy in firsts:
        copy.wait_recv()
    acc = jnp.zeros(out1.shape, F32)
    for i in range(n_plane):
        acc = acc + g1p[i].astype(F32)
    g1d[dpi] = acc.astype(BF16)
    last = spread(nd, dp_id, held(g1d, dpi), g1d.at[dpi], dp_send, dp_recv, 1)
    sent += last

    for copy in gather:
        copy.wait_recv()
    for i in range(n_plane):
        out2[i * rows : (i + 1) * rows] = ag[i].astype(F32)
    for copy in last:
        copy.wait_recv()
    acc = jnp.zeros(out1.shape, F32)
    for i in range(nd):
        acc = acc + g1d[i].astype(F32)
    out1[...] = acc
    for copy, dx, dy in halos:
        pl.when(there(dx, dy))(copy.wait_send)
    for copy in sent:
        copy.wait_send()


def shards(nd, nx, ny, volume, first_weight, second_weight, cotangent):
    _, chans, X, Y, Z = volume.shape
    inner, outer = first_weight.shape[0], second_weight.shape[0]
    width = second_weight.shape[1]
    hx, hy, hz = X // 2, Y // 2, Z // 2
    cells = hx * hy
    n_plane = nx * ny
    rows = outer // n_plane
    tap_rows = -(-3 * chans // 16) * 16
    vmem = pl.BlockSpec(memory_space=pltpu.VMEM)
    dma = pltpu.SemaphoreType.DMA
    return pl.pallas_call(
        functools.partial(kernel, nd, nx, ny),
        out_shape=(
            jax.ShapeDtypeStruct(first_weight.shape, F32),
            jax.ShapeDtypeStruct(second_weight.shape, F32),
        ),
        in_specs=[pl.BlockSpec(memory_space=pltpu.HBM)] * 4,
        out_specs=(vmem, vmem),
        scratch_shapes=[
            pltpu.VMEM(volume.shape, BF16),
            pltpu.VMEM(first_weight.shape, BF16),
            pltpu.VMEM(second_weight.shape, BF16),
            pltpu.VMEM(cotangent.shape, BF16),
            pltpu.VMEM((8,) + volume.shape[1:], BF16),
            pltpu.VMEM(((X + 2 * REACH) * 3 * Y * tap_rows, Z), F32),
            pltpu.VMEM((X + 2 * REACH, Y + 2 * REACH, tap_rows, Z), BF16),
            pltpu.VMEM((outer * cells, hz), F32),
            pltpu.VMEM((outer, cells * Z), F32),
            pltpu.VMEM((hx + 2, hy + 2, 3 * inner, Z), BF16),
            pltpu.VMEM((hx + 2, hy + 2, inner, Z), F32),
            pltpu.VMEM((X + 4, inner, (Y + 4) * Z), F32),
            pltpu.VMEM((width, outer), BF16),
            pltpu.VMEM((n_plane, rows, width), BF16),
            pltpu.VMEM((n_plane, rows, width), BF16),
            pltpu.VMEM((nd, rows, width), BF16),
            pltpu.VMEM((n_plane, rows, width), BF16),
            pltpu.VMEM((n_plane,) + first_weight.shape, BF16),
            pltpu.VMEM((nd,) + first_weight.shape, BF16),
            dma((8,)),
            dma((8,)),
            dma((3, n_plane)),
            dma((3, n_plane)),
            dma((2, nd)),
            dma((2, nd)),
            dma((4,)),
        ],
        compiler_params=pltpu.CompilerParams(
            collective_id=0, has_side_effects=True, vmem_limit_bytes=60 * 1024 * 1024
        ),
        name="step",
    )(volume, first_weight, second_weight, cotangent)


def solution(mesh):
    sizes = dict(mesh.shape)
    return jax.shard_map(
        functools.partial(shards, sizes["dp"], sizes["sx"], sizes["sy"]),
        mesh=mesh,
        in_specs=(P("dp", None, "sx", "sy", None), P(), P(), P("dp", None, "sx", "sy", None)),
        out_specs=(P(), P()),
        check_vma=False,
    )
```

```python
import functools

import jax
import jax.numpy as jnp
from jax import lax
from jax.experimental import pallas as pl
from jax.experimental.pallas import tpu as pltpu
from jax.sharding import PartitionSpec as P

F32 = jnp.float32
BF16 = jnp.bfloat16
MESH = pl.DeviceIdType.MESH
REACH = 3
DIRS = [(dx, dy) for dx in (-1, 0, 1) for dy in (-1, 0, 1) if (dx, dy) != (0, 0)]


def nt(a, b):
    return lax.dot_general(a, b, (((1,), (1,)), ((), ())), preferred_element_type=F32)


def nn(a, b):
    return jnp.dot(a, b, preferred_element_type=F32)


def iota(shape, dim):
    return lax.broadcasted_iota(jnp.int32, shape, dim)


def one_hot(cond):
    return jnp.where(cond, 1.0, 0.0).astype(BF16)


def slope(value):
    return 0.65 + 0.35 * jnp.tanh(0.5 * value)


def leaky(value):
    tail = jnp.log(1.0 + jnp.exp(-jnp.abs(value)))
    return 0.3 * value + 0.7 * (jnp.maximum(value, 0.0) + tail)


def kernel(
    nd, nx, ny,
    vol_h, w1_h, w2_h, cot_h,
    out1, out2,
    vol, w1, w2, cot,
    raw, rows_f, vs, cot_f, cot_d, q, ups, slope1, w2t,
    g2s, g2r, g2d, ag, g1p, g1d,
    halo_send, halo_recv, plane_send, plane_recv, dp_send, dp_recv, fetch_sem,
):
    fetches = [
        pltpu.make_async_copy(src, dst, fetch_sem.at[i])
        for i, (src, dst) in enumerate(((vol_h, vol), (w1_h, w1), (w2_h, w2), (cot_h, cot)))
    ]
    for fetch in fetches:
        fetch.start()
    dpi, ix, iy = lax.axis_index("dp"), lax.axis_index("sx"), lax.axis_index("sy")
    n_plane = nx * ny
    me = ix * ny + iy
    chans, X, Y, Z = vol.shape[1:]
    hx, hy, hz = X // 2, Y // 2, Z // 2
    inner, outer = w1.shape[0], w2.shape[0]
    rows = outer // n_plane
    taps = 3 * chans
    tap_rows = vs.shape[2]

    raw[...] = jnp.zeros_like(raw)

    def plane_id(r):
        peer = lax.rem(me + r, n_plane)
        return {"sx": peer // ny, "sy": lax.rem(peer, ny)}

    def dp_id(r):
        return {"dp": lax.rem(dpi + r, nd)}

    barrier = pltpu.get_barrier_semaphore()
    for r in range(1, n_plane):
        pl.semaphore_signal(barrier, inc=1, device_id=plane_id(r), device_id_type=MESH)
    for r in range(1, nd):
        pl.semaphore_signal(barrier, inc=1, device_id=dp_id(r), device_id_type=MESH)

    def inside(d, i, n):
        return (i + d >= 0) & (i + d < n)

    def there(dx, dy):
        if dx == 0:
            return inside(dy, iy, ny)
        if dy == 0:
            return inside(dx, ix, nx)
        return inside(dx, ix, nx) & inside(dy, iy, ny)

    def xs(dx):
        return {-1: range(X - REACH, X), 0: range(X), 1: range(REACH)}[dx]

    halos = []
    for i, (dx, dy) in enumerate(DIRS):
        span = xs(-dx)
        part = pl.ds(span[0], len(span))
        copy = pltpu.make_async_remote_copy(
            src_ref=vol.at[0, :, part],
            dst_ref=raw.at[DIRS.index((-dx, -dy)), :, part],
            send_sem=halo_send.at[i],
            recv_sem=halo_recv.at[i],
            device_id={"sx": ix + dx, "sy": iy + dy},
            device_id_type=MESH,
        )
        halos.append((copy, dx, dy))

    rows_f[...] = jnp.zeros_like(rows_f)
    fetches[0].wait()
    pl.semaphore_wait(barrier, n_plane - 1 + nd - 1)
    for copy, dx, dy in halos:
        pl.when(there(dx, dy))(copy.start)

    def spread(count, ids, src, dst, send, recv, stage):
        copies = []
        for r in range(1, count):
            copy = pltpu.make_async_remote_copy(
                src_ref=src(r),
                dst_ref=dst,
                send_sem=send.at[stage, r],
                recv_sem=recv.at[stage, r],
                device_id=ids(r),
                device_id_type=MESH,
            )
            copy.start()
            copies.append(copy)
        return copies

    lane = iota((Y, Z), 1)

    def lay(src, dx, dy):
        for c in range(chans):
            for x in xs(dx):
                v = src(c, x).astype(F32)
                down = jnp.where(lane == 0, 0.0, pltpu.roll(v, 1, 1))
                up_z = jnp.where(lane == Z - 1, 0.0, pltpu.roll(v, Z - 1, 1))
                first = ((x + dx * X + REACH) * 3 + dy + 1) * Y
                for e, moved in enumerate((down, v, up_z)):
                    at = first * tap_rows + e * chans + c
                    rows_f[pl.ds(at, Y, stride=tap_rows), :] = moved

    def pack(x, y):
        start = (x * 3 * Y + y + Y - REACH) * tap_rows
        vs[x, y] = rows_f[start : start + tap_rows].astype(BF16)

    lay(lambda c, x: vol[0, c, x], 0, 0)
    own = [(x, y) for x in range(REACH, X + REACH) for y in range(REACH, Y + REACH)]
    for x, y in own:
        pack(x, y)
    for fetch in fetches[1:]:
        fetch.wait()
    n12 = 9 * taps
    pick_r, pick_c = iota((n12, 9 * tap_rows), 0), iota((n12, 9 * tap_rows), 1)
    tap = lax.rem(pick_c, tap_rows)
    pick = one_hot((pick_r == (pick_c // tap_rows) * taps + tap) & (tap < taps))
    w1p = nn(w1[...], pick).astype(BF16)
    eye = one_hot(iota((128, 128), 0) == iota((128, 128), 1))
    width = w2.shape[1]
    for at in range(0, width, 128):
        n = min(128, width - at)
        w2t[at : at + n] = nt(eye[:n, :n], w2[:, at : at + n]).astype(BF16)
    for o in range(outer):
        for x in range(hx):
            start = (o * hx + x) * hy
            cot_f[start : start + hy] = cot[0, o, x].astype(F32)
    cells = hx * hy
    stack = jnp.concatenate(
        [cot_f[pl.ds(i, outer, stride=cells), :] for i in range(cells)], axis=0
    ).astype(BF16)
    double = one_hot(iota((hz, Z), 0) == iota((hz, Z), 1) // 2)
    doubled = nn(stack, double)
    for i in range(cells):
        cot_d[:, i * Z : (i + 1) * Z] = doubled[i * outer : (i + 1) * outer]
    p_in, p_out = iota((4 * Z, 3 * Z), 0), iota((4 * Z, 3 * Z), 1)
    pool_m = one_hot(
        lax.rem(p_in, Z) // 2 == lax.rem(p_out, Z) // 2 + p_out // Z - 1
    )
    t_in, t_out = iota((Z, 2 * Z), 0), iota((Z, 2 * Z), 1)
    shift_m = one_hot(t_in == jnp.where(t_out < Z, t_out + 2, t_out - Z - 2))

    def present(d, i, n):
        return jnp.where(inside(d, i, n), 1.0, 0.0) if d else 1.0

    in_x = {d: present(d, ix, nx) for d in (-1, 0, 1)}
    in_y = {d: present(d, iy, ny) for d in (-1, 0, 1)}

    def part_of(at, rim, size):
        return -1 if at < rim else (1 if at >= rim + size else 0)

    def masked(value, at_x, at_y):
        if at_x:
            value = value * in_x[at_x]
        if at_y:
            value = value * in_y[at_y]
        return value

    for copy, dx, dy in halos:
        pl.when(there(-dx, -dy))(copy.wait_recv)
    for i, (dx, dy) in enumerate(DIRS):
        lay(lambda c, x, i=i: raw[i, c, x], dx, dy)
    for x in range(X + 2 * REACH):
        for y in range(Y + 2 * REACH):
            if (x, y) not in own:
                pack(x, y)

    wide, high = X + 4, Y + 4

    def fine_cols(x):
        return jnp.concatenate(
            [
                jnp.concatenate([vs[x + a, y + b] for y in range(high)], axis=1)
                for a in range(3)
                for b in range(3)
            ],
            axis=0,
        )

    for xc in range(hx + 2):
        hid = []
        for x in (2 * xc, 2 * xc + 1):
            pre = nn(w1p, fine_cols(x))
            slope1[x] = pre
            hid.append(leaky(pre).astype(BF16))
        block = jnp.concatenate(
            [
                jnp.concatenate(
                    [
                        hid[i][:, (2 * yc + j) * Z : (2 * yc + j + 1) * Z]
                        for i in range(2)
                        for j in range(2)
                    ],
                    axis=1,
                )
                for yc in range(hy + 2)
            ],
            axis=0,
        )
        mean = nn(block, pool_m) * 0.125
        for yc in range(hy + 2):
            tile = mean[yc * inner : (yc + 1) * inner]
            tile = masked(tile, part_of(xc, 1, hx), part_of(yc, 1, hy)).astype(BF16)
            for e in range(3):
                q[xc, yc, e * inner : (e + 1) * inner] = tile[:, e * Z : (e + 1) * Z]

    places = [(x, y) for x in range(hx) for y in range(hy)]

    def coarse_cols():
        return jnp.concatenate(
            [
                jnp.concatenate([q[x + a, y + b] for x, y in places], axis=1)
                for a in range(3)
                for b in range(3)
            ],
            axis=0,
        )

    pre_second = nn(w2[...], coarse_cols())
    back = (cot_d[...] * slope(pre_second)).astype(BF16)

    count = cells * hz * nd * n_plane
    scale_second, scale_first = count**-0.5, (8 * count) ** -0.5
    grad2 = nt(back, coarse_cols()) * (0.5 * scale_second)
    for i in range(n_plane):
        g2s[i] = grad2[i * rows : (i + 1) * rows].astype(BF16)
    g2r[me] = g2s[me]
    in_plane = lambda r: g2s.at[lax.rem(me + r, n_plane)]
    scatter = spread(n_plane, plane_id, in_plane, g2r.at[me], plane_send, plane_recv, 0)
    sent = list(scatter)

    tiles = jnp.concatenate([back[:, i * Z : (i + 1) * Z] for i in range(cells)], axis=0)
    moved = nn(tiles, shift_m).astype(BF16)

    def flat(value, half):
        return jnp.concatenate(
            [
                value[i * outer : (i + 1) * outer, half * Z : (half + 1) * Z]
                for i in range(cells)
            ],
            axis=1,
        )

    share = None
    for e, rhs in enumerate((flat(moved, 0), back, flat(moved, 1))):
        lhs = jnp.concatenate(
            [w2t[(3 * ab + e) * inner : (3 * ab + e + 1) * inner] for ab in range(9)],
            axis=0,
        )
        term = nn(lhs, rhs)
        share = term if share is None else share + term
    for xe in range(hx + 2):
        for ye in range(hy + 2):
            total = None
            for a in range(3):
                for b in range(3):
                    x, y = xe - a, ye - b
                    if 0 <= x < hx and 0 <= y < hy:
                        ab, at = 3 * a + b, (x * hy + y) * Z
                        term = share[ab * inner : (ab + 1) * inner, at : at + Z]
                        total = term if total is None else total + term
            ups[xe, ye] = masked(total * 0.125, part_of(xe, 1, hx), part_of(ye, 1, hy))

    for x in range(wide):
        slope1[x] = slope(slope1[x])

    held = lambda ref, i: (lambda r: ref.at[i])
    grad1 = jnp.zeros((inner, 9 * tap_rows), F32)
    for x in range(wide):
        low = jnp.concatenate(
            [ups[x // 2, y // 2] * slope1[x, :, y * Z : (y + 1) * Z] for y in range(high)],
            axis=1,
        ).astype(BF16)
        grad1 = grad1 + nt(low, fine_cols(x))
    grad1 = nt((grad1 * scale_first).astype(BF16), pick)
    g1p[me] = grad1.astype(BF16)
    firsts = spread(n_plane, plane_id, held(g1p, me), g1p.at[me], plane_send, plane_recv, 1)
    sent += firsts

    for copy in scatter:
        copy.wait_recv()
    acc = jnp.zeros((rows, width), F32)
    for i in range(n_plane):
        acc = acc + g2r[i].astype(F32)
    g2d[dpi] = acc.astype(BF16)
    across = spread(nd, dp_id, held(g2d, dpi), g2d.at[dpi], dp_send, dp_recv, 0)
    sent += across

    for copy in across:
        copy.wait_recv()
    acc = jnp.zeros((rows, width), F32)
    for i in range(nd):
        acc = acc + g2d[i].astype(F32)
    ag[me] = acc.astype(BF16)
    gather = spread(n_plane, plane_id, held(ag, me), ag.at[me], plane_send, plane_recv, 2)
    sent += gather

    for copy in firsts:
        copy.wait_recv()
    acc = jnp.zeros(out1.shape, F32)
    for i in range(n_plane):
        acc = acc + g1p[i].astype(F32)
    g1d[dpi] = acc.astype(BF16)
    last = spread(nd, dp_id, held(g1d, dpi), g1d.at[dpi], dp_send, dp_recv, 1)
    sent += last

    for copy in gather:
        copy.wait_recv()
    for i in range(n_plane):
        out2[i * rows : (i + 1) * rows] = ag[i].astype(F32)
    for copy in last:
        copy.wait_recv()
    acc = jnp.zeros(out1.shape, F32)
    for i in range(nd):
        acc = acc + g1d[i].astype(F32)
    out1[...] = acc
    for copy, dx, dy in halos:
        pl.when(there(dx, dy))(copy.wait_send)
    for copy in sent:
        copy.wait_send()


def shards(nd, nx, ny, volume, first_weight, second_weight, cotangent):
    _, chans, X, Y, Z = volume.shape
    inner, outer = first_weight.shape[0], second_weight.shape[0]
    width = second_weight.shape[1]
    hx, hy, hz = X // 2, Y // 2, Z // 2
    cells = hx * hy
    n_plane = nx * ny
    rows = outer // n_plane
    tap_rows = -(-3 * chans // 16) * 16
    vmem = pl.BlockSpec(memory_space=pltpu.VMEM)
    dma = pltpu.SemaphoreType.DMA
    return pl.pallas_call(
        functools.partial(kernel, nd, nx, ny),
        out_shape=(
            pltpu.VMEM(first_weight.shape, F32),
            pltpu.VMEM(second_weight.shape, F32),
        ),
        in_specs=[pl.BlockSpec(memory_space=pltpu.HBM)] * 4,
        out_specs=(vmem, vmem),
        scratch_shapes=[
            pltpu.VMEM(volume.shape, BF16),
            pltpu.VMEM(first_weight.shape, BF16),
            pltpu.VMEM(second_weight.shape, BF16),
            pltpu.VMEM(cotangent.shape, BF16),
            pltpu.VMEM((8,) + volume.shape[1:], BF16),
            pltpu.VMEM(((X + 2 * REACH) * 3 * Y * tap_rows, Z), F32),
            pltpu.VMEM((X + 2 * REACH, Y + 2 * REACH, tap_rows, Z), BF16),
            pltpu.VMEM((outer * cells, hz), F32),
            pltpu.VMEM((outer, cells * Z), F32),
            pltpu.VMEM((hx + 2, hy + 2, 3 * inner, Z), BF16),
            pltpu.VMEM((hx + 2, hy + 2, inner, Z), F32),
            pltpu.VMEM((X + 4, inner, (Y + 4) * Z), F32),
            pltpu.VMEM((width, outer), BF16),
            pltpu.VMEM((n_plane, rows, width), BF16),
            pltpu.VMEM((n_plane, rows, width), BF16),
            pltpu.VMEM((nd, rows, width), BF16),
            pltpu.VMEM((n_plane, rows, width), BF16),
            pltpu.VMEM((n_plane,) + first_weight.shape, BF16),
            pltpu.VMEM((nd,) + first_weight.shape, BF16),
            dma((8,)),
            dma((8,)),
            dma((3, n_plane)),
            dma((3, n_plane)),
            dma((2, nd)),
            dma((2, nd)),
            dma((4,)),
        ],
        compiler_params=pltpu.CompilerParams(
            collective_id=0, has_side_effects=True, vmem_limit_bytes=57000 * 1024
        ),
        name="step",
    )(volume, first_weight, second_weight, cotangent)


def solution(mesh):
    sizes = dict(mesh.shape)
    return jax.shard_map(
        functools.partial(shards, sizes["dp"], sizes["sx"], sizes["sy"]),
        mesh=mesh,
        in_specs=(P("dp", None, "sx", "sy", None), P(), P(), P("dp", None, "sx", "sy", None)),
        out_specs=(P(), P()),
        check_vma=False,
    )
```

```python
import functools

import jax
import jax.numpy as jnp
from jax import lax
from jax.experimental import pallas as pl
from jax.experimental.pallas import tpu as pltpu
from jax.sharding import PartitionSpec as P

F32 = jnp.float32
BF16 = jnp.bfloat16
MESH = pl.DeviceIdType.MESH
REACH = 3
DIRS = [(dx, dy) for dx in (-1, 0, 1) for dy in (-1, 0, 1) if (dx, dy) != (0, 0)]


def nt(a, b):
    return lax.dot_general(a, b, (((1,), (1,)), ((), ())), preferred_element_type=F32)


def nn(a, b):
    return jnp.dot(a, b, preferred_element_type=F32)


def iota(shape, dim):
    return lax.broadcasted_iota(jnp.int32, shape, dim)


def one_hot(cond):
    return jnp.where(cond, 1.0, 0.0).astype(BF16)


def slope(value):
    return 0.65 + 0.35 * jnp.tanh(0.5 * value)


def leaky(value):
    tail = jnp.log(1.0 + jnp.exp(-jnp.abs(value)))
    return 0.3 * value + 0.7 * (jnp.maximum(value, 0.0) + tail)


def kernel(
    nd, nx, ny,
    vol_h, w1_h, w2_h, cot_h,
    out1, out2,
    vol, w1, w2, cot,
    raw, rows_f, vs, cot_f, cot_d, q, ups, slope1, w2t,
    g2s, g2r, g2d, ag, g1p, g1d,
    halo_send, halo_recv, plane_send, plane_recv, dp_send, dp_recv, fetch_sem,
):
    fetches = [
        pltpu.make_async_copy(src, dst, fetch_sem.at[i])
        for i, (src, dst) in enumerate(((vol_h, vol), (w1_h, w1), (w2_h, w2), (cot_h, cot)))
    ]
    for fetch in fetches:
        fetch.start()
    dpi, ix, iy = lax.axis_index("dp"), lax.axis_index("sx"), lax.axis_index("sy")
    n_plane = nx * ny
    me = ix * ny + iy
    chans, X, Y, Z = vol.shape[1:]
    hx, hy, hz = X // 2, Y // 2, Z // 2
    inner, outer = w1.shape[0], w2.shape[0]
    rows = outer // n_plane
    taps = 3 * chans
    tap_rows = vs.shape[2]

    raw[...] = jnp.zeros_like(raw)

    def plane_id(r):
        peer = lax.rem(me + r, n_plane)
        return {"sx": peer // ny, "sy": lax.rem(peer, ny)}

    def dp_id(r):
        return {"dp": lax.rem(dpi + r, nd)}

    barrier = pltpu.get_barrier_semaphore()
    for r in range(1, n_plane):
        pl.semaphore_signal(barrier, inc=1, device_id=plane_id(r), device_id_type=MESH)
    for r in range(1, nd):
        pl.semaphore_signal(barrier, inc=1, device_id=dp_id(r), device_id_type=MESH)

    def inside(d, i, n):
        return (i + d >= 0) & (i + d < n)

    def there(dx, dy):
        if dx == 0:
            return inside(dy, iy, ny)
        if dy == 0:
            return inside(dx, ix, nx)
        return inside(dx, ix, nx) & inside(dy, iy, ny)

    def xs(dx):
        return {-1: range(X - REACH, X), 0: range(X), 1: range(REACH)}[dx]

    halos = []
    for i, (dx, dy) in enumerate(DIRS):
        span = xs(-dx)
        part = pl.ds(span[0], len(span))
        copy = pltpu.make_async_remote_copy(
            src_ref=vol.at[0, :, part],
            dst_ref=raw.at[DIRS.index((-dx, -dy)), :, part],
            send_sem=halo_send.at[i],
            recv_sem=halo_recv.at[i],
            device_id={"sx": ix + dx, "sy": iy + dy},
            device_id_type=MESH,
        )
        halos.append((copy, dx, dy))

    rows_f[...] = jnp.zeros_like(rows_f)
    fetches[0].wait()
    pl.semaphore_wait(barrier, n_plane - 1 + nd - 1)
    for copy, dx, dy in halos:
        pl.when(there(dx, dy))(copy.start)

    def spread(count, ids, src, dst, send, recv, stage):
        copies = []
        for r in range(1, count):
            copy = pltpu.make_async_remote_copy(
                src_ref=src(r),
                dst_ref=dst,
                send_sem=send.at[stage, r],
                recv_sem=recv.at[stage, r],
                device_id=ids(r),
                device_id_type=MESH,
            )
            copy.start()
            copies.append(copy)
        return copies

    lane = iota((Y, Z), 1)

    def lay(src, dx, dy):
        for c in range(chans):
            for x in xs(dx):
                v = src(c, x).astype(F32)
                down = jnp.where(lane == 0, 0.0, pltpu.roll(v, 1, 1))
                up_z = jnp.where(lane == Z - 1, 0.0, pltpu.roll(v, Z - 1, 1))
                first = ((x + dx * X + REACH) * 3 + dy + 1) * Y
                for e, moved in enumerate((down, v, up_z)):
                    at = first * tap_rows + e * chans + c
                    rows_f[pl.ds(at, Y, stride=tap_rows), :] = moved

    def pack(x, y):
        start = (x * 3 * Y + y + Y - REACH) * tap_rows
        vs[x, y] = rows_f[start : start + tap_rows].astype(BF16)

    lay(lambda c, x: vol[0, c, x], 0, 0)
    own = [(x, y) for x in range(REACH, X + REACH) for y in range(REACH, Y + REACH)]
    for x, y in own:
        pack(x, y)
    for fetch in fetches[1:]:
        fetch.wait()
    n12 = 9 * taps
    pick_r, pick_c = iota((n12, 9 * tap_rows), 0), iota((n12, 9 * tap_rows), 1)
    tap = lax.rem(pick_c, tap_rows)
    pick = one_hot((pick_r == (pick_c // tap_rows) * taps + tap) & (tap < taps))
    w1p = nn(w1[...], pick).astype(BF16)
    eye = one_hot(iota((128, 128), 0) == iota((128, 128), 1))
    width = w2.shape[1]
    for at in range(0, width, 128):
        n = min(128, width - at)
        w2t[at : at + n] = nt(eye[:n, :n], w2[:, at : at + n]).astype(BF16)
    for o in range(outer):
        for x in range(hx):
            start = (o * hx + x) * hy
            cot_f[start : start + hy] = cot[0, o, x].astype(F32)
    cells = hx * hy
    stack = jnp.concatenate(
        [cot_f[pl.ds(i, outer, stride=cells), :] for i in range(cells)], axis=0
    ).astype(BF16)
    double = one_hot(iota((hz, Z), 0) == iota((hz, Z), 1) // 2)
    doubled = nn(stack, double)
    for i in range(cells):
        cot_d[:, i * Z : (i + 1) * Z] = doubled[i * outer : (i + 1) * outer]
    p_in, p_out = iota((4 * Z, 3 * Z), 0), iota((4 * Z, 3 * Z), 1)
    pool_m = one_hot(
        lax.rem(p_in, Z) // 2 == lax.rem(p_out, Z) // 2 + p_out // Z - 1
    )
    t_in, t_out = iota((Z, 2 * Z), 0), iota((Z, 2 * Z), 1)
    shift_m = one_hot(t_in == jnp.where(t_out < Z, t_out + 2, t_out - Z - 2))

    def present(d, i, n):
        return jnp.where(inside(d, i, n), 1.0, 0.0) if d else 1.0

    in_x = {d: present(d, ix, nx) for d in (-1, 0, 1)}
    in_y = {d: present(d, iy, ny) for d in (-1, 0, 1)}

    def part_of(at, rim, size):
        return -1 if at < rim else (1 if at >= rim + size else 0)

    def masked(value, at_x, at_y):
        if at_x:
            value = value * in_x[at_x]
        if at_y:
            value = value * in_y[at_y]
        return value

    for copy, dx, dy in halos:
        pl.when(there(-dx, -dy))(copy.wait_recv)
    for i, (dx, dy) in enumerate(DIRS):
        lay(lambda c, x, i=i: raw[i, c, x], dx, dy)
    for x in range(X + 2 * REACH):
        for y in range(Y + 2 * REACH):
            if (x, y) not in own:
                pack(x, y)

    wide, high = X + 4, Y + 4

    def fine_cols(x):
        return jnp.concatenate(
            [
                jnp.concatenate([vs[x + a, y + b] for y in range(high)], axis=1)
                for a in range(3)
                for b in range(3)
            ],
            axis=0,
        )

    for xc in range(hx + 2):
        hid = []
        for x in (2 * xc, 2 * xc + 1):
            pre = nn(w1p, fine_cols(x))
            slope1[x] = pre
            hid.append(leaky(pre).astype(BF16))
        block = jnp.concatenate(
            [
                jnp.concatenate(
                    [
                        hid[i][:, (2 * yc + j) * Z : (2 * yc + j + 1) * Z]
                        for i in range(2)
                        for j in range(2)
                    ],
                    axis=1,
                )
                for yc in range(hy + 2)
            ],
            axis=0,
        )
        mean = nn(block, pool_m) * 0.125
        for yc in range(hy + 2):
            tile = mean[yc * inner : (yc + 1) * inner]
            tile = masked(tile, part_of(xc, 1, hx), part_of(yc, 1, hy)).astype(BF16)
            for e in range(3):
                q[xc, yc, e * inner : (e + 1) * inner] = tile[:, e * Z : (e + 1) * Z]

    places = [(x, y) for x in range(hx) for y in range(hy)]

    def coarse_cols():
        return jnp.concatenate(
            [
                jnp.concatenate([q[x + a, y + b] for x, y in places], axis=1)
                for a in range(3)
                for b in range(3)
            ],
            axis=0,
        )

    pre_second = nn(w2[...], coarse_cols())
    back = (cot_d[...] * slope(pre_second)).astype(BF16)

    count = cells * hz * nd * n_plane
    scale_second, scale_first = count**-0.5, (8 * count) ** -0.5
    grad2 = nt(back, coarse_cols()) * (0.5 * scale_second)
    for i in range(n_plane):
        g2s[i] = grad2[i * rows : (i + 1) * rows].astype(BF16)
    g2r[me] = g2s[me]
    in_plane = lambda r: g2s.at[lax.rem(me + r, n_plane)]
    scatter = spread(n_plane, plane_id, in_plane, g2r.at[me], plane_send, plane_recv, 0)
    sent = list(scatter)

    tiles = jnp.concatenate([back[:, i * Z : (i + 1) * Z] for i in range(cells)], axis=0)
    moved = nn(tiles, shift_m).astype(BF16)

    def flat(value, half):
        return jnp.concatenate(
            [
                value[i * outer : (i + 1) * outer, half * Z : (half + 1) * Z]
                for i in range(cells)
            ],
            axis=1,
        )

    share = None
    for e, rhs in enumerate((flat(moved, 0), back, flat(moved, 1))):
        lhs = jnp.concatenate(
            [w2t[(3 * ab + e) * inner : (3 * ab + e + 1) * inner] for ab in range(9)],
            axis=0,
        )
        term = nn(lhs, rhs)
        share = term if share is None else share + term
    for xe in range(hx + 2):
        for ye in range(hy + 2):
            total = None
            for a in range(3):
                for b in range(3):
                    x, y = xe - a, ye - b
                    if 0 <= x < hx and 0 <= y < hy:
                        ab, at = 3 * a + b, (x * hy + y) * Z
                        term = share[ab * inner : (ab + 1) * inner, at : at + Z]
                        total = term if total is None else total + term
            ups[xe, ye] = masked(total * 0.125, part_of(xe, 1, hx), part_of(ye, 1, hy))

    for x in range(wide):
        slope1[x] = slope(slope1[x])

    held = lambda ref, i: (lambda r: ref.at[i])
    grad1 = jnp.zeros((inner, 9 * tap_rows), F32)
    for x in range(wide):
        low = jnp.concatenate(
            [ups[x // 2, y // 2] * slope1[x, :, y * Z : (y + 1) * Z] for y in range(high)],
            axis=1,
        ).astype(BF16)
        grad1 = grad1 + nt(low, fine_cols(x))
    grad1 = nt((grad1 * scale_first).astype(BF16), pick)
    g1p[me] = grad1.astype(BF16)
    firsts = spread(n_plane, plane_id, held(g1p, me), g1p.at[me], plane_send, plane_recv, 1)
    sent += firsts

    for copy in scatter:
        copy.wait_recv()
    acc = jnp.zeros((rows, width), F32)
    for i in range(n_plane):
        acc = acc + g2r[i].astype(F32)
    g2d[dpi] = acc.astype(BF16)
    across = spread(nd, dp_id, held(g2d, dpi), g2d.at[dpi], dp_send, dp_recv, 0)
    sent += across

    for copy in across:
        copy.wait_recv()
    acc = jnp.zeros((rows, width), F32)
    for i in range(nd):
        acc = acc + g2d[i].astype(F32)
    ag[me] = acc.astype(BF16)
    gather = spread(n_plane, plane_id, held(ag, me), ag.at[me], plane_send, plane_recv, 2)
    sent += gather

    for copy in firsts:
        copy.wait_recv()
    acc = jnp.zeros(out1.shape, F32)
    for i in range(n_plane):
        acc = acc + g1p[i].astype(F32)
    g1d[dpi] = acc.astype(BF16)
    last = spread(nd, dp_id, held(g1d, dpi), g1d.at[dpi], dp_send, dp_recv, 1)
    sent += last

    for copy in gather:
        copy.wait_recv()
    for i in range(n_plane):
        out2[i * rows : (i + 1) * rows] = ag[i].astype(F32)
    for copy in last:
        copy.wait_recv()
    acc = jnp.zeros(out1.shape, F32)
    for i in range(nd):
        acc = acc + g1d[i].astype(F32)
    out1[...] = acc
    for copy, dx, dy in halos:
        pl.when(there(dx, dy))(copy.wait_send)
    for copy in sent:
        copy.wait_send()


def put_out(first, second, out1, out2, sem):
    copies = [
        pltpu.make_async_copy(src, dst, sem.at[i])
        for i, (src, dst) in enumerate(((second, out2), (first, out1)))
    ]
    for copy in copies:
        copy.start()
    for copy in copies:
        copy.wait()


def shards(nd, nx, ny, volume, first_weight, second_weight, cotangent):
    _, chans, X, Y, Z = volume.shape
    inner, outer = first_weight.shape[0], second_weight.shape[0]
    width = second_weight.shape[1]
    hx, hy, hz = X // 2, Y // 2, Z // 2
    cells = hx * hy
    n_plane = nx * ny
    rows = outer // n_plane
    tap_rows = -(-3 * chans // 16) * 16
    vmem = pl.BlockSpec(memory_space=pltpu.VMEM)
    dma = pltpu.SemaphoreType.DMA
    grads = pl.pallas_call(
        functools.partial(kernel, nd, nx, ny),
        out_shape=(
            pltpu.VMEM(first_weight.shape, F32),
            pltpu.VMEM(second_weight.shape, F32),
        ),
        in_specs=[pl.BlockSpec(memory_space=pltpu.HBM)] * 4,
        out_specs=(vmem, vmem),
        scratch_shapes=[
            pltpu.VMEM(volume.shape, BF16),
            pltpu.VMEM(first_weight.shape, BF16),
            pltpu.VMEM(second_weight.shape, BF16),
            pltpu.VMEM(cotangent.shape, BF16),
            pltpu.VMEM((8,) + volume.shape[1:], BF16),
            pltpu.VMEM(((X + 2 * REACH) * 3 * Y * tap_rows, Z), F32),
            pltpu.VMEM((X + 2 * REACH, Y + 2 * REACH, tap_rows, Z), BF16),
            pltpu.VMEM((outer * cells, hz), F32),
            pltpu.VMEM((outer, cells * Z), F32),
            pltpu.VMEM((hx + 2, hy + 2, 3 * inner, Z), BF16),
            pltpu.VMEM((hx + 2, hy + 2, inner, Z), F32),
            pltpu.VMEM((X + 4, inner, (Y + 4) * Z), F32),
            pltpu.VMEM((width, outer), BF16),
            pltpu.VMEM((n_plane, rows, width), BF16),
            pltpu.VMEM((n_plane, rows, width), BF16),
            pltpu.VMEM((nd, rows, width), BF16),
            pltpu.VMEM((n_plane, rows, width), BF16),
            pltpu.VMEM((n_plane,) + first_weight.shape, BF16),
            pltpu.VMEM((nd,) + first_weight.shape, BF16),
            dma((8,)),
            dma((8,)),
            dma((3, n_plane)),
            dma((3, n_plane)),
            dma((2, nd)),
            dma((2, nd)),
            dma((4,)),
        ],
        compiler_params=pltpu.CompilerParams(
            collective_id=0, has_side_effects=True, vmem_limit_bytes=57000 * 1024
        ),
        name="step",
    )(volume, first_weight, second_weight, cotangent)
    return pl.pallas_call(
        put_out,
        out_shape=tuple(jax.ShapeDtypeStruct(g.shape, F32) for g in grads),
        in_specs=[vmem] * 2,
        out_specs=(pl.BlockSpec(memory_space=pltpu.HBM),) * 2,
        scratch_shapes=[dma((2,))],
        compiler_params=pltpu.CompilerParams(vmem_limit_bytes=4 * 1024 * 1024),
        name="put_out",
    )(*grads)


def solution(mesh):
    sizes = dict(mesh.shape)
    return jax.shard_map(
        functools.partial(shards, sizes["dp"], sizes["sx"], sizes["sy"]),
        mesh=mesh,
        in_specs=(P("dp", None, "sx", "sy", None), P(), P(), P("dp", None, "sx", "sy", None)),
        out_specs=(P(), P()),
        check_vma=False,
    )
```
